32 devices in a mesh: replica: 8 (over z, core), tp: 4 (over y, x).
Axes of the slice: x: 2, y: 2, z: 4, core: 2. Of those that a mesh axis runs over, the one named last changes fastest.
Arguments:
- token_ids: int32 [128], replicated, may hold values from 0 to 8191
- embed_table: bfloat16 [8192, 8192], P('replica', 'tp'), may hold values from -6 to 6
- norm_gain: bfloat16 [8192], replicated, may hold values from 0.099609375 to 1.8984375
- w_query: bfloat16 [8192, 4096], P(('replica', 'tp')), may hold values from -0.0625 to 0.0625
- w_keyvalue: bfloat16 [8192, 2, 512], P(('replica', 'tp')), may hold values from -0.0625 to 0.0625
- key_cache: bfloat16 [512, 1024, 128], P(('replica', 'tp')), may hold values from -360 to 360
- value_cache: bfloat16 [512, 1024, 128], P(('replica', 'tp')), may hold values from -6 to 6
- cache_lengths: int32 [128], P('replica'), may hold values from 1 to 1024, as said below
Outputs:
- context: bfloat16 [512, 1024], P(('replica', 'tp'))
- query_weight_tp: bfloat16 [8192, 4096], P(None, 'tp')
- keyvalue_weight_tp: bfloat16 [8192, 2, 512], P(None, None, 'tp')
The draws below stay inside these ranges and needn't reach their ends.
Inputs may be any that keep to these rules, and one draw needn't show every extreme that they name: `cache_lengths`: some sequence has exactly 1024 filled slots.
All inputs are finite; a program needn't handle non-finite values.
Results may differ from the reference program's by a relative error of at most 0.019.
The reference program's roundings to bfloat16 on the way count: a program that leaves them out, or rounds other values in their place, can miss the bound.
Values may be sent and summed in bfloat16 or wider, within the bound.
A program may use at most 128 MiB of HBM per device.

```python
import math
import jax
import jax.numpy as jnp
import numpy as np
from jax import lax

D = 8192
HD = 128
QHEADS = 32
KVHEADS = 4
BATCH = 16
CTX = 1024
VOCAB = 8192
GROUP = 8
SEQS = 128
CACHE_ROWS = 512
N_REPLICA = 8


def draw_key_cache(key, part):
    base = jnp.clip(jax.random.normal(key, (CACHE_ROWS, CTX, HD), jnp.float32), -6.0, 6.0)
    return base.astype(jnp.bfloat16)


def draw_cache_lengths(key, part):
    lengths = jax.random.randint(key, (SEQS,), 1, CTX + 1, jnp.int32)
    chosen = jax.random.randint(jax.random.fold_in(key, 3), (), 0, SEQS, jnp.int32)
    return jnp.where(jnp.arange(SEQS, dtype=jnp.int32) == chosen, CTX, lengths).astype(jnp.int32)


def plant(array, key, low, high):
    dims = array.shape
    spot = [jax.random.randint(jax.random.fold_in(key, axis), (), 0, dims[axis]) for axis in range(len(dims))]
    array = array.at[tuple(spot)].set(low)
    longest = dims.index(max(dims))
    spot[longest] = (spot[longest] + 1) % dims[longest]
    return array.at[tuple(spot)].set(high)


def level_of(stream_key, extent, pieces, least, largest):
    level = 1.0
    for dim, shards_of in pieces:
        heights = jax.random.uniform(jax.random.fold_in(jax.random.fold_in(stream_key, 6), dim), (shards_of,), jnp.float32, least / len(pieces), largest / len(pieces))
        level = level * jnp.repeat(jnp.exp(heights), extent[dim] // shards_of).reshape((-1,) + (1,) * (len(extent) - 1 - dim))
    return level


def rank_bounds(amount, skew):
    weights = [(1 << 20) // math.isqrt(grade ** skew) + 1 for grade in range(1, amount + 1)]
    spread = 1 + sum(weights) // (1 << 30)
    return np.cumsum(np.array([max(1, weight // spread) for weight in weights]))


def ranked(key, dims, number_of, skew):
    listing = rank_bounds(number_of, skew)
    ticket = jax.random.randint(jax.random.fold_in(key, 1), dims, 0, int(listing[number_of - 1]))
    grade = jnp.searchsorted(jnp.asarray(listing, jnp.int32), ticket, side="right")
    return jax.random.permutation(jax.random.fold_in(key, 2), number_of)[grade].astype(jnp.int32)


def normal_values(own_key, extent, width, limit, shards=(), held_as=jnp.bfloat16):
    gain = level_of(own_key, extent, shards, -0.22, 0.18) if shards else 1.0
    array = jax.random.normal(own_key, extent, jnp.float32) * width * gain
    return jnp.minimum(jnp.maximum(array, -limit), limit).astype(held_as)


def setup_inputs(seed: int = 0) -> dict:
    arg_keys = jax.random.split(jax.random.key(seed), 9)
    return {
        "token_ids": plant(ranked(arg_keys[0], (SEQS,), VOCAB, 2), jax.random.fold_in(arg_keys[0], 3), 0, VOCAB - 1).astype(jnp.int32),
        "embed_table": normal_values(arg_keys[1], (VOCAB, D), 1.0, 6.0, ((0, 8), (1, 4))),
        "norm_gain": jnp.clip(1.0 + 0.18 * jax.random.normal(arg_keys[2], (D,), jnp.float32), 0.099609375, 1.8984375).astype(jnp.bfloat16),
        "w_query": normal_values(arg_keys[3], (D, QHEADS * HD), D ** -0.5, 0.0625, ((0, 32),)),
        "w_keyvalue": normal_values(arg_keys[4], (D, 2, KVHEADS * HD), D ** -0.5, 0.0625, ((0, 32),)),
        "key_cache": draw_key_cache(jax.random.fold_in(arg_keys[8], 71), 0),
        "value_cache": normal_values(arg_keys[6], (CACHE_ROWS, CTX, HD), 1.0, 6.0, ((0, 32),)),
        "cache_lengths": draw_cache_lengths(jax.random.fold_in(arg_keys[8], 71), 0),
    }


def attend(query, keys, values, key_new, value_new, lengths):
    scale = query.shape[-1] ** (-0.5)
    scores = jnp.einsum('rgd,rcd->rgc', query.astype(jnp.float32), keys.astype(jnp.float32)) * scale
    position = lax.broadcasted_iota(jnp.int32, scores.shape, 2)
    scores = jnp.where(position < lengths[:, None, None], scores, -jnp.inf)
    own = jnp.einsum('rgd,rd->rg', query.astype(jnp.float32), key_new.astype(jnp.float32)) * scale
    top = jnp.maximum(lax.optimization_barrier(jnp.max(scores, axis=2)), own)
    weights = jnp.exp(scores - top[:, :, None])
    own_weight = jnp.exp(own - top)
    total = lax.optimization_barrier(jnp.sum(weights, axis=2)) + own_weight
    weights = (weights / total[:, :, None]).astype(jnp.bfloat16)
    own_weight = (own_weight / total).astype(jnp.bfloat16)
    context = jnp.einsum('rgc,rcd->rgd', weights.astype(jnp.float32), values.astype(jnp.float32))
    context = context + own_weight.astype(jnp.float32)[:, :, None] * value_new.astype(jnp.float32)[:, None, :]
    return context.astype(jnp.bfloat16)

def reference(token_ids, embed_table, norm_gain, w_query, w_keyvalue, key_cache, value_cache, cache_lengths):
    query_weight_tp = w_query
    keyvalue_weight_tp = w_keyvalue
    embedded = jnp.take(embed_table, token_ids, axis=0)
    values32 = embedded.astype(jnp.float32)
    mean_square = lax.optimization_barrier(jnp.mean(values32 * values32, axis=1, keepdims=True))
    normed = (values32 * lax.rsqrt(mean_square + 1e-05) * norm_gain.astype(jnp.float32)).astype(jnp.bfloat16)
    query = jnp.dot(normed, w_query, preferred_element_type=jnp.float32).astype(jnp.bfloat16)
    pair = jnp.dot(normed, w_keyvalue.reshape(D, 2 * KVHEADS * HD), preferred_element_type=jnp.float32).astype(jnp.bfloat16)
    pair = pair.reshape(SEQS, 2, KVHEADS * HD)
    query = query.reshape(N_REPLICA, BATCH, KVHEADS, GROUP, HD).transpose(0, 2, 1, 3, 4).reshape(N_REPLICA, KVHEADS * BATCH, GROUP, HD)
    key_new = pair[:, 0].reshape(N_REPLICA, BATCH, KVHEADS, HD).transpose(0, 2, 1, 3).reshape(N_REPLICA, KVHEADS * BATCH, HD)
    value_new = pair[:, 1].reshape(N_REPLICA, BATCH, KVHEADS, HD).transpose(0, 2, 1, 3).reshape(N_REPLICA, KVHEADS * BATCH, HD)
    keys = key_cache.reshape(N_REPLICA, KVHEADS * BATCH, CTX, HD)
    values = value_cache.reshape(N_REPLICA, KVHEADS * BATCH, CTX, HD)
    lengths = jnp.tile(cache_lengths.reshape(N_REPLICA, BATCH), (1, KVHEADS))

    def per_group(items):
        return attend(items[0], items[1], items[2], items[3], items[4], items[5])
    context = lax.map(per_group, (query, keys, values, key_new, value_new, lengths))
    context = context.reshape(CACHE_ROWS, GROUP * HD)
    return (context, query_weight_tp, keyvalue_weight_tp)
```

```python
import functools

import jax
import jax.numpy as jnp
from jax import lax
from jax.experimental import pallas as pl
from jax.experimental.pallas import tpu as pltpu
from jax.sharding import PartitionSpec as P


def attend(query, keys, values, key_new, value_new, lengths):
    scale = query.shape[-1] ** (-0.5)
    scores = jnp.einsum("rgd,rcd->rgc", query, keys, preferred_element_type=jnp.float32) * scale
    position = lax.broadcasted_iota(jnp.int32, scores.shape, 2)
    scores = jnp.where(position < lengths[:, None, None], scores, -jnp.inf)
    own = jnp.einsum("rgd,rd->rg", query, key_new, preferred_element_type=jnp.float32) * scale
    top = jnp.maximum(jnp.max(scores, axis=2), own)
    weights = jnp.exp(scores - top[:, :, None])
    own_weight = jnp.exp(own - top)
    total = jnp.sum(weights, axis=2) + own_weight
    weights = (weights / total[:, :, None]).astype(jnp.bfloat16)
    own_weight = (own_weight / total).astype(jnp.bfloat16)
    context = jnp.einsum("rgc,rcd->rgd", weights, values, preferred_element_type=jnp.float32)
    context = (
        context
        + own_weight.astype(jnp.float32)[:, :, None] * value_new.astype(jnp.float32)[:, None, :]
    )
    return context.astype(jnp.bfloat16)


def per_device(
    token_ids, embed_table, norm_gain, w_query, w_keyvalue, key_cache, value_cache, cache_lengths
):
    group_index = lax.axis_index("replica")
    tp_index = lax.axis_index("tp")
    vocab_rows, feature_cols = embed_table.shape
    batch = cache_lengths.shape[0]
    first_id = group_index * vocab_rows
    picked = token_ids - first_id
    columns = lax.broadcasted_iota(jnp.int32, (batch * lax.axis_size("replica"), vocab_rows), 1)
    onehot = (picked[:, None] == columns).astype(jnp.bfloat16)
    embedded = lax.psum_scatter(
        jnp.dot(onehot, embed_table, preferred_element_type=jnp.float32),
        "replica",
        scatter_dimension=0,
        tiled=True,
    ).astype(jnp.bfloat16)
    whole = lax.all_gather(embedded, "tp", axis=1, tiled=True)
    values32 = whole.astype(jnp.float32)
    mean_square = jnp.mean(values32 * values32, axis=1, keepdims=True)
    normed = (values32 * lax.rsqrt(mean_square + 1e-05) * norm_gain.astype(jnp.float32)).astype(
        jnp.bfloat16
    )
    width = normed.shape[1]
    query_rows = w_query.reshape(w_query.shape[0], 1, w_query.shape[1])
    query_mid, pair_mid = (
        lax.all_to_all(query_rows, "tp", split_axis=2, concat_axis=0, tiled=True),
        lax.all_to_all(w_keyvalue, "tp", split_axis=2, concat_axis=0, tiled=True),
    )
    flat_query = query_mid.reshape(query_mid.shape[0], query_mid.shape[2])
    pair_cols = pair_mid.shape[2]
    flat_pair = pair_mid.reshape(pair_mid.shape[0], 2 * pair_cols)
    query_full, pair_full = (
        lax.all_gather(flat_query, "replica", axis=0, tiled=True),
        lax.all_gather(flat_pair, "replica", axis=0, tiled=True),
    )
    query_acc = jnp.dot(normed, query_full, preferred_element_type=jnp.float32)
    pair_acc = jnp.dot(normed, pair_full, preferred_element_type=jnp.float32)
    query_local = query_acc.astype(jnp.bfloat16)
    pair_local = pair_acc.astype(jnp.bfloat16).reshape(batch, 2, pair_cols)
    query_heads, pair_heads = (
        lax.all_gather(query_local, "tp", axis=1, tiled=True),
        lax.all_gather(pair_local, "tp", axis=2, tiled=True),
    )
    head_size = key_cache.shape[2]
    kv_heads = pair_heads.shape[2] // head_size
    group = query_heads.shape[1] // (kv_heads * head_size)
    rows_here = key_cache.shape[0]
    first_row = tp_index * rows_here
    query_grouped = (
        query_heads.reshape(batch, kv_heads, group, head_size)
        .transpose(1, 0, 2, 3)
        .reshape(kv_heads * batch, group, head_size)
    )
    key_grouped = (
        pair_heads[:, 0]
        .reshape(batch, kv_heads, head_size)
        .transpose(1, 0, 2)
        .reshape(kv_heads * batch, head_size)
    )
    value_grouped = (
        pair_heads[:, 1]
        .reshape(batch, kv_heads, head_size)
        .transpose(1, 0, 2)
        .reshape(kv_heads * batch, head_size)
    )
    query_mine = lax.dynamic_slice_in_dim(query_grouped, first_row, rows_here, 0)
    key_mine = lax.dynamic_slice_in_dim(key_grouped, first_row, rows_here, 0)
    value_mine = lax.dynamic_slice_in_dim(value_grouped, first_row, rows_here, 0)
    sequence = (first_row + lax.broadcasted_iota(jnp.int32, (rows_here,), 0)) % batch
    matches = sequence[:, None] == lax.broadcasted_iota(jnp.int32, (rows_here, batch), 1)
    row_lengths = jnp.sum(jnp.where(matches, cache_lengths[None, :], 0), axis=1)
    context = attend(query_mine, key_cache, value_cache, key_mine, value_mine, row_lengths)
    context = context.reshape(rows_here, group * head_size)
    return (context, query_full, pair_full.reshape(width, 2, pair_cols))


MESH = pl.DeviceIdType.MESH


def exchange_kernel(
    planes,
    part_ref,
    gain_ref,
    query_ref,
    pair_ref,
    query_out,
    pair_out,
    normed_ref,
    spread_ref,
    query_hold,
    pair_hold,
    picked,
    pieces,
    send_sem,
    recv_sem,
    plane_sem,
    local_sem,
    pick_send,
    pick_recv,
    piece_send,
    piece_recv,
):
    r, t = lax.axis_index("replica"), lax.axis_index("tp")
    replicas = 2 * planes
    z, k = r // 2, lax.rem(r, 2)
    ty, tx = t // 2, lax.rem(t, 2)
    rows, query_cols = query_hold.shape
    pair_cols = pair_hold.shape[2]
    batch, feats = picked.shape[1], picked.shape[2]
    other = [t, ty * 2 + 1 - tx, (1 - ty) * 2 + tx, 3 - t]
    partner = z * 2 + 1 - k
    width = replicas * 4 * rows

    barrier = pltpu.get_barrier_semaphore()
    for step in range(1, replicas):
        pl.semaphore_signal(
            barrier, inc=1, device_id=(lax.rem(r + step, replicas), t), device_id_type=MESH
        )
    for j in range(1, 4):
        pl.semaphore_signal(barrier, inc=1, device_id=(r, other[j]), device_id_type=MESH)
    pl.semaphore_wait(barrier, replicas - 1 + 3)

    def piece_id(plane, core, tp):
        return (plane * 2 + core) * 4 + tp

    def rows_of(ref, pid):
        where = pl.ds(pl.multiple_of(pid * rows, rows), rows)
        return ref.at[where]

    def columns(tp):
        return (
            query_ref.at[:, pl.ds(pl.multiple_of(tp * query_cols, query_cols), query_cols)],
            pair_ref.at[:, :, pl.ds(pl.multiple_of(tp * pair_cols, pair_cols), pair_cols)],
        )

    def copies(pid, sources, way, slot, target):
        made = []
        for c, (source, out) in enumerate(zip(sources, (query_out, pair_out))):
            sem = plane_sem.at[c, slot] if way is None else send_sem.at[c, way, slot]
            made.append(
                pltpu.make_async_remote_copy(
                    src_ref=source,
                    dst_ref=rows_of(out, pid),
                    send_sem=sem,
                    recv_sem=recv_sem.at[c, pid],
                    device_id=target,
                    device_id_type=MESH,
                )
            )
        return made

    def landed(pid):
        for c, out in enumerate((query_out, pair_out)):
            pltpu.make_async_copy(
                rows_of(out, pid), rows_of(out, pid), recv_sem.at[c, pid]
            ).wait()

    def onward(pid, sources, slot, up, down, wait=False):
        def act(made):
            for copy in made:
                copy.wait_send() if wait else copy.start()

        if up:

            @pl.when(z < planes - 1)
            def _():
                act(copies(pid, sources, 0, slot, (lax.rem(r + 2, replicas), t)))

        if down:

            @pl.when(z > 0)
            def _():
                act(copies(pid, sources, 1, slot, (lax.rem(r + replicas - 2, replicas), t)))

        act(copies(pid, sources, 2, slot, (partner, t)))

    def stored(pid):
        return rows_of(query_out, pid), rows_of(pair_out, pid)

    mine = piece_id(z, k, t)
    sources = columns(t)
    bring = [
        pltpu.make_async_copy(sources[0], query_hold, local_sem.at[0]),
        pltpu.make_async_copy(sources[1], pair_hold, local_sem.at[1]),
    ]
    across = [copies(mine, columns(other[j]), None, j - 1, (r, other[j])) for j in range(1, 4)]
    for made in across:
        for copy in made:
            copy.start()
    onward(mine, sources, 0, True, True)
    for copy in bring:
        copy.start()

    def batch_rows(replica):
        return part_ref.at[pl.ds(pl.multiple_of(replica * batch, batch), batch)]

    keep = pltpu.make_async_copy(batch_rows(r), picked.at[r], local_sem.at[2])
    keep.start()
    picks = []
    for step in range(1, replicas):
        target = lax.rem(r + step, replicas)
        picks.append(
            pltpu.make_async_remote_copy(
                src_ref=batch_rows(target),
                dst_ref=picked.at[r],
                send_sem=pick_send.at[step],
                recv_sem=pick_recv.at[step],
                device_id=(target, t),
                device_id_type=MESH,
            )
        )
    for copy in picks:
        copy.start()
    for copy in bring:
        copy.wait()
    put = [
        pltpu.make_async_copy(query_hold, rows_of(query_out, mine), local_sem.at[3]),
        pltpu.make_async_copy(pair_hold, rows_of(pair_out, mine), local_sem.at[4]),
    ]
    for copy in put:
        copy.start()

    gather = [
        pltpu.make_async_remote_copy(
            src_ref=pieces.at[t],
            dst_ref=pieces.at[t],
            send_sem=piece_send.at[j - 1],
            recv_sem=piece_recv.at[j - 1],
            device_id=(r, other[j]),
            device_id_type=MESH,
        )
        for j in range(1, 4)
    ]

    def sum_picks():
        keep.wait()
        for copy in picks:
            copy.wait()
        total = picked[0].astype(jnp.float32)
        for step in range(1, replicas):
            total = total + picked[step].astype(jnp.float32)
        pieces[t] = total.astype(jnp.bfloat16)

    def normalise():
        for copy in gather:
            copy.wait()
        square = jnp.zeros((batch, 1), jnp.float32)
        for i in range(4):
            part = pieces[i].astype(jnp.float32)
            square = square + jnp.sum(part * part, axis=1, keepdims=True)
        factor = lax.rsqrt(square / (4 * feats) + 1e-05)
        for i in range(4):
            part = pieces[i].astype(jnp.float32)
            gain = gain_ref[:, i * feats : (i + 1) * feats].astype(jnp.float32)
            normed_ref[:, i * feats : (i + 1) * feats] = (part * factor * gain).astype(
                jnp.bfloat16
            )
        block = 256
        line = lax.broadcasted_iota(jnp.int32, (block, 2 * block), 0)
        column = lax.broadcasted_iota(jnp.int32, (block, 2 * block), 1)
        even = (column == 2 * line).astype(jnp.bfloat16)
        odd = (column == 2 * line + 1).astype(jnp.bfloat16)

        def spread(i, carry):
            part = normed_ref[:, pl.ds(pl.multiple_of(i * block, block), block)]
            where = pl.ds(pl.multiple_of(i * 2 * block, 2 * block), 2 * block)
            spread_ref[0:batch, where] = jnp.dot(
                part, even, preferred_element_type=jnp.float32
            ).astype(jnp.bfloat16)
            spread_ref[batch : 2 * batch, where] = jnp.dot(
                part, odd, preferred_element_type=jnp.float32
            ).astype(jnp.bfloat16)
            return carry

        lax.fori_loop(0, 4 * feats // block, spread, 0)

    steps = 4 * (planes - 1)
    for step in range(steps):
        if 0 < step < 4:
            pid = piece_id(z, k, other[step])
            landed(pid)
            onward(pid, stored(pid), step, True, True)
        far, j = step // 4 + 1, step % 4

        @pl.when(z >= far)
        def _():
            pid = piece_id(lax.rem(z + planes - far, planes), k, other[j])
            landed(pid)
            onward(pid, stored(pid), 4 * far + j, True, False)

        @pl.when(z + far < planes)
        def _():
            pid = piece_id(lax.rem(z + far, planes), k, other[j])
            landed(pid)
            onward(pid, stored(pid), 4 * (planes - 1 + far) + j, False, True)

        if step == 5:
            sum_picks()
        if step == 7:
            for copy in gather:
                copy.start()
        if step == 8:
            normalise()

    for copy in put:
        copy.wait()
    for made in across:
        for copy in made:
            copy.wait_send()
    onward(mine, sources, 0, True, True, wait=True)
    for j in range(1, 4):
        pid = piece_id(z, k, other[j])
        onward(pid, stored(pid), j, True, True, wait=True)
    for step in range(steps):
        far, j = step // 4 + 1, step % 4

        @pl.when(z >= far)
        def _():
            pid = piece_id(lax.rem(z + planes - far, planes), k, other[j])
            onward(pid, stored(pid), 4 * far + j, True, False, wait=True)

        @pl.when(z + far < planes)
        def _():
            pid = piece_id(lax.rem(z + far, planes), k, other[j])
            onward(pid, stored(pid), 4 * (planes - 1 + far) + j, False, True, wait=True)

    for plane in range(planes):
        for j in range(4):
            landed(piece_id(plane, 1 - k, j))


def exchange(part, norm_gain, w_query, w_keyvalue, planes, batch):
    rows, all_query = w_query.shape
    query_cols, pair_cols = all_query // 4, w_keyvalue.shape[2] // 4
    replicas = 2 * planes
    width = rows * replicas * 4
    feats = part.shape[1]
    anywhere = pl.BlockSpec(memory_space=pl.ANY)
    vmem = pl.BlockSpec(memory_space=pltpu.VMEM)
    dma = pltpu.SemaphoreType.DMA
    slots = 4 * (2 * planes - 1)
    return pl.pallas_call(
        functools.partial(exchange_kernel, planes),
        out_shape=(
            jax.ShapeDtypeStruct((width, query_cols), w_query.dtype),
            jax.ShapeDtypeStruct((width, 2, pair_cols), w_query.dtype),
            jax.ShapeDtypeStruct((batch, width), w_query.dtype),
            jax.ShapeDtypeStruct((2 * batch, 2 * width), w_query.dtype),
        ),
        in_specs=[anywhere, vmem, anywhere, anywhere],
        out_specs=(anywhere, anywhere, vmem, vmem),
        scratch_shapes=[
            pltpu.VMEM((rows, query_cols), w_query.dtype),
            pltpu.VMEM((rows, 2, pair_cols), w_query.dtype),
            pltpu.VMEM((replicas, batch, feats), part.dtype),
            pltpu.VMEM((4, batch, feats), part.dtype),
            dma((2, 3, slots)),
            dma((2, replicas * 4)),
            dma((2, 3)),
            dma((5,)),
            dma((replicas,)),
            dma((replicas,)),
            dma((3,)),
            dma((3,)),
        ],
        compiler_params=pltpu.CompilerParams(
            collective_id=0, has_side_effects=True, vmem_limit_bytes=12 * 2**20
        ),
        cost_estimate=pl.CostEstimate(
            flops=2 * 10**11, bytes_accessed=2 * width * query_cols, transcendentals=0
        ),
        name="weight_exchange",
    )(part, norm_gain.reshape(1, -1), w_query, w_keyvalue)


def project_kernel(
    normed_ref, spread_ref, query_in, pair_in, query_ref, pair_ref, q_ref, kv_ref, q_acc, kv_acc
):
    step = pl.program_id(0)

    @pl.when(step == 0)
    def _():
        q_acc[...] = jnp.zeros_like(q_acc)
        kv_acc[...] = jnp.zeros_like(kv_acc)

    query_ref[...] = query_in[...]
    pair_ref[...] = pair_in[...]
    q_acc[...] += jnp.dot(normed_ref[...], query_in[...], preferred_element_type=jnp.float32)
    kv_acc[...] += jnp.dot(spread_ref[...], pair_in[...], preferred_element_type=jnp.float32)

    @pl.when(step == pl.num_programs(0) - 1)
    def _():
        q_ref[...] = q_acc[...].astype(q_ref.dtype)
        kv_ref[...] = kv_acc[...].astype(kv_ref.dtype)


def project(normed, spread, query_all, pair_all):
    batch, width = normed.shape
    query_cols, pair_cols = query_all.shape[1], pair_all.shape[2]
    pair_flat = pair_all.reshape(2 * width, pair_cols)
    block = 512
    query_spec = pl.BlockSpec((block, query_cols), lambda i: (i, 0))
    pair_spec = pl.BlockSpec((2 * block, pair_cols), lambda i: (i, 0))
    query_out, pair_out, query, pair = pl.pallas_call(
        project_kernel,
        grid=(width // block,),
        out_shape=(
            jax.ShapeDtypeStruct(query_all.shape, query_all.dtype),
            jax.ShapeDtypeStruct(pair_flat.shape, pair_all.dtype),
            jax.ShapeDtypeStruct((batch, query_cols), normed.dtype),
            jax.ShapeDtypeStruct((2 * batch, pair_cols), normed.dtype),
        ),
        in_specs=[
            pl.BlockSpec((batch, block), lambda i: (0, i)),
            pl.BlockSpec((2 * batch, 2 * block), lambda i: (0, i)),
            query_spec,
            pair_spec,
        ],
        out_specs=(
            query_spec,
            pair_spec,
            pl.BlockSpec((batch, query_cols), lambda i: (0, 0)),
            pl.BlockSpec((2 * batch, pair_cols), lambda i: (0, 0)),
        ),
        scratch_shapes=[
            pltpu.VMEM((batch, query_cols), jnp.float32),
            pltpu.VMEM((2 * batch, pair_cols), jnp.float32),
        ],
        compiler_params=pltpu.CompilerParams(vmem_limit_bytes=16 * 2**20),
        cost_estimate=pl.CostEstimate(
            flops=2 * batch * width * (query_cols + 4 * pair_cols),
            bytes_accessed=4 * width * (query_cols + 2 * pair_cols),
            transcendentals=0,
        ),
        name="project_and_store",
    )(normed, spread, query_all, pair_flat)
    return query_out, pair_out.reshape(width, 2, pair_cols), query, pair


def per_device_line(
    planes,
    token_ids,
    embed_table,
    norm_gain,
    w_query,
    w_keyvalue,
    key_cache,
    value_cache,
    cache_lengths,
):
    vocab_rows = embed_table.shape[0]
    batch = cache_lengths.shape[0]
    head_size = key_cache.shape[2]
    picked = token_ids - lax.axis_index("replica") * vocab_rows
    columns = lax.broadcasted_iota(jnp.int32, (token_ids.shape[0], vocab_rows), 1)
    onehot = (picked[:, None] == columns).astype(jnp.bfloat16)
    part = jnp.dot(onehot, embed_table, preferred_element_type=jnp.float32).astype(jnp.bfloat16)
    query_all, pair_all, normed, spread = exchange(
        part, norm_gain, w_query, w_keyvalue, planes, batch
    )
    query_out, pair_out, query, pair = project(normed, spread, query_all, pair_all)
    query = query.reshape(batch, -1, head_size)
    context = attend(query, key_cache, value_cache, pair[:batch], pair[batch:], cache_lengths)
    return context.reshape(batch, -1), query_out, pair_out


def solution(mesh):
    replicas, tp = mesh.shape["replica"], mesh.shape["tp"]

    def body(*args):
        key_cache, lengths, w_keyvalue = args[5], args[7], args[4]
        one_head = w_keyvalue.shape[2] == tp * key_cache.shape[2]
        own_rows = key_cache.shape[0] == lengths.shape[0]
        if tp == 4 and replicas % 2 == 0 and replicas > 6 and one_head and own_rows:
            return per_device_line(replicas // 2, *args)
        return per_device(*args)

    return jax.shard_map(
        body,
        mesh=mesh,
        in_specs=(
            P(),
            P("replica", "tp"),
            P(),
            P(("replica", "tp"), None),
            P(("replica", "tp"), None, None),
            P(("replica", "tp"), None, None),
            P(("replica", "tp"), None, None),
            P("replica"),
        ),
        out_specs=(P(("replica", "tp"), None), P(None, "tp"), P(None, None, "tp")),
        check_vma=False,
    )
```

```python
import functools

import jax
import jax.numpy as jnp
from jax import lax
from jax.experimental import pallas as pl
from jax.experimental.pallas import tpu as pltpu
from jax.sharding import PartitionSpec as P


def attend(query, keys, values, key_new, value_new, lengths):
    scale = query.shape[-1] ** (-0.5)
    scores = jnp.einsum("rgd,rcd->rgc", query, keys, preferred_element_type=jnp.float32) * scale
    position = lax.broadcasted_iota(jnp.int32, scores.shape, 2)
    scores = jnp.where(position < lengths[:, None, None], scores, -jnp.inf)
    own = jnp.einsum("rgd,rd->rg", query, key_new, preferred_element_type=jnp.float32) * scale
    top = jnp.maximum(jnp.max(scores, axis=2), own)
    weights = jnp.exp(scores - top[:, :, None])
    own_weight = jnp.exp(own - top)
    total = jnp.sum(weights, axis=2) + own_weight
    weights = (weights / total[:, :, None]).astype(jnp.bfloat16)
    own_weight = (own_weight / total).astype(jnp.bfloat16)
    context = jnp.einsum("rgc,rcd->rgd", weights, values, preferred_element_type=jnp.float32)
    context = (
        context
        + own_weight.astype(jnp.float32)[:, :, None] * value_new.astype(jnp.float32)[:, None, :]
    )
    return context.astype(jnp.bfloat16)


def per_device(
    token_ids, embed_table, norm_gain, w_query, w_keyvalue, key_cache, value_cache, cache_lengths
):
    group_index = lax.axis_index("replica")
    tp_index = lax.axis_index("tp")
    vocab_rows, feature_cols = embed_table.shape
    batch = cache_lengths.shape[0]
    first_id = group_index * vocab_rows
    picked = token_ids - first_id
    columns = lax.broadcasted_iota(jnp.int32, (batch * lax.axis_size("replica"), vocab_rows), 1)
    onehot = (picked[:, None] == columns).astype(jnp.bfloat16)
    embedded = lax.psum_scatter(
        jnp.dot(onehot, embed_table, preferred_element_type=jnp.float32),
        "replica",
        scatter_dimension=0,
        tiled=True,
    ).astype(jnp.bfloat16)
    whole = lax.all_gather(embedded, "tp", axis=1, tiled=True)
    values32 = whole.astype(jnp.float32)
    mean_square = jnp.mean(values32 * values32, axis=1, keepdims=True)
    normed = (values32 * lax.rsqrt(mean_square + 1e-05) * norm_gain.astype(jnp.float32)).astype(
        jnp.bfloat16
    )
    width = normed.shape[1]
    query_rows = w_query.reshape(w_query.shape[0], 1, w_query.shape[1])
    query_mid, pair_mid = (
        lax.all_to_all(query_rows, "tp", split_axis=2, concat_axis=0, tiled=True),
        lax.all_to_all(w_keyvalue, "tp", split_axis=2, concat_axis=0, tiled=True),
    )
    flat_query = query_mid.reshape(query_mid.shape[0], query_mid.shape[2])
    pair_cols = pair_mid.shape[2]
    flat_pair = pair_mid.reshape(pair_mid.shape[0], 2 * pair_cols)
    query_full, pair_full = (
        lax.all_gather(flat_query, "replica", axis=0, tiled=True),
        lax.all_gather(flat_pair, "replica", axis=0, tiled=True),
    )
    query_acc = jnp.dot(normed, query_full, preferred_element_type=jnp.float32)
    pair_acc = jnp.dot(normed, pair_full, preferred_element_type=jnp.float32)
    query_local = query_acc.astype(jnp.bfloat16)
    pair_local = pair_acc.astype(jnp.bfloat16).reshape(batch, 2, pair_cols)
    query_heads, pair_heads = (
        lax.all_gather(query_local, "tp", axis=1, tiled=True),
        lax.all_gather(pair_local, "tp", axis=2, tiled=True),
    )
    head_size = key_cache.shape[2]
    kv_heads = pair_heads.shape[2] // head_size
    group = query_heads.shape[1] // (kv_heads * head_size)
    rows_here = key_cache.shape[0]
    first_row = tp_index * rows_here
    query_grouped = (
        query_heads.reshape(batch, kv_heads, group, head_size)
        .transpose(1, 0, 2, 3)
        .reshape(kv_heads * batch, group, head_size)
    )
    key_grouped = (
        pair_heads[:, 0]
        .reshape(batch, kv_heads, head_size)
        .transpose(1, 0, 2)
        .reshape(kv_heads * batch, head_size)
    )
    value_grouped = (
        pair_heads[:, 1]
        .reshape(batch, kv_heads, head_size)
        .transpose(1, 0, 2)
        .reshape(kv_heads * batch, head_size)
    )
    query_mine = lax.dynamic_slice_in_dim(query_grouped, first_row, rows_here, 0)
    key_mine = lax.dynamic_slice_in_dim(key_grouped, first_row, rows_here, 0)
    value_mine = lax.dynamic_slice_in_dim(value_grouped, first_row, rows_here, 0)
    sequence = (first_row + lax.broadcasted_iota(jnp.int32, (rows_here,), 0)) % batch
    matches = sequence[:, None] == lax.broadcasted_iota(jnp.int32, (rows_here, batch), 1)
    row_lengths = jnp.sum(jnp.where(matches, cache_lengths[None, :], 0), axis=1)
    context = attend(query_mine, key_cache, value_cache, key_mine, value_mine, row_lengths)
    context = context.reshape(rows_here, group * head_size)
    return (context, query_full, pair_full.reshape(width, 2, pair_cols))


MESH = pl.DeviceIdType.MESH


def exchange_kernel(
    planes,
    token_ref,
    gain_ref,
    table_ref,
    query_ref,
    pair_ref,
    query_out,
    pair_out,
    normed_ref,
    spread_ref,
    query_hold,
    pair_hold,
    table_hold,
    part_ref,
    given,
    joined,
    picked,
    pieces,
    send_sem,
    recv_sem,
    plane_sem,
    local_sem,
    give_send,
    give_recv,
    pick_send,
    pick_recv,
    piece_send,
    piece_recv,
):
    r, t = lax.axis_index("replica"), lax.axis_index("tp")
    replicas = 2 * planes
    z, k = r // 2, lax.rem(r, 2)
    ty, tx = t // 2, lax.rem(t, 2)
    rows, query_cols = query_hold.shape
    pair_cols = pair_hold.shape[2]
    batch, feats = picked.shape[1], picked.shape[2]
    other = [t, ty * 2 + 1 - tx, (1 - ty) * 2 + tx, 3 - t]
    partner = z * 2 + 1 - k
    width = replicas * 4 * rows

    barrier = pltpu.get_barrier_semaphore()
    for step in range(1, replicas):
        pl.semaphore_signal(
            barrier, inc=1, device_id=(lax.rem(r + step, replicas), t), device_id_type=MESH
        )
    for j in range(1, 4):
        pl.semaphore_signal(barrier, inc=1, device_id=(r, other[j]), device_id_type=MESH)
    pl.semaphore_wait(barrier, replicas - 1 + 3)

    def piece_id(plane, core, tp):
        return (plane * 2 + core) * 4 + tp

    def rows_of(ref, pid):
        where = pl.ds(pl.multiple_of(pid * rows, rows), rows)
        return ref.at[where]

    def columns(tp):
        return (
            query_ref.at[:, pl.ds(pl.multiple_of(tp * query_cols, query_cols), query_cols)],
            pair_ref.at[:, :, pl.ds(pl.multiple_of(tp * pair_cols, pair_cols), pair_cols)],
        )

    def copies(pid, sources, way, slot, target):
        made = []
        for c, (source, out) in enumerate(zip(sources, (query_out, pair_out))):
            sem = plane_sem.at[c, slot] if way is None else send_sem.at[c, way, slot]
            made.append(
                pltpu.make_async_remote_copy(
                    src_ref=source,
                    dst_ref=rows_of(out, pid),
                    send_sem=sem,
                    recv_sem=recv_sem.at[c, pid],
                    device_id=target,
                    device_id_type=MESH,
                )
            )
        return made

    def landed(pid):
        for c, out in enumerate((query_out, pair_out)):
            pltpu.make_async_copy(
                rows_of(out, pid), rows_of(out, pid), recv_sem.at[c, pid]
            ).wait()

    def onward(pid, sources, slot, up, down, wait=False):
        def act(made):
            for copy in made:
                copy.wait_send() if wait else copy.start()

        if up:

            @pl.when(z < planes - 1)
            def _():
                act(copies(pid, sources, 0, slot, (lax.rem(r + 2, replicas), t)))

        if down:

            @pl.when(z > 0)
            def _():
                act(copies(pid, sources, 1, slot, (lax.rem(r + replicas - 2, replicas), t)))

        act(copies(pid, sources, 2, slot, (partner, t)))

    def stored(pid):
        return rows_of(query_out, pid), rows_of(pair_out, pid)

    mine = piece_id(z, k, t)
    sources = columns(t)
    bring = [
        pltpu.make_async_copy(sources[0], query_hold, local_sem.at[0]),
        pltpu.make_async_copy(sources[1], pair_hold, local_sem.at[1]),
    ]
    across = [copies(mine, columns(other[j]), None, j - 1, (r, other[j])) for j in range(1, 4)]
    for made in across:
        for copy in made:
            copy.start()
    onward(mine, sources, 0, True, True)
    for copy in bring:
        copy.start()

    table = pltpu.make_async_copy(table_ref, table_hold, local_sem.at[2])
    table.start()
    gives = [
        pltpu.make_async_remote_copy(
            src_ref=part_ref.at[plane, 1 - k],
            dst_ref=given.at[plane],
            send_sem=give_send.at[plane],
            recv_sem=give_recv.at[plane],
            device_id=(partner, t),
            device_id_type=MESH,
        )
        for plane in range(planes)
    ]
    picks = []
    for far in range(1, planes):
        plane = lax.rem(z + far, planes)
        picks.append(
            pltpu.make_async_remote_copy(
                src_ref=joined.at[plane],
                dst_ref=picked.at[far - 1],
                send_sem=pick_send.at[far - 1],
                recv_sem=pick_recv.at[far - 1],
                device_id=(plane * 2 + k, t),
                device_id_type=MESH,
            )
        )
    for copy in bring:
        copy.wait()
    put = [
        pltpu.make_async_copy(query_hold, rows_of(query_out, mine), local_sem.at[3]),
        pltpu.make_async_copy(pair_hold, rows_of(pair_out, mine), local_sem.at[4]),
    ]
    for copy in put:
        copy.start()

    gather = [
        pltpu.make_async_remote_copy(
            src_ref=pieces.at[t],
            dst_ref=pieces.at[t],
            send_sem=piece_send.at[j - 1],
            recv_sem=piece_recv.at[j - 1],
            device_id=(r, other[j]),
            device_id_type=MESH,
        )
        for j in range(1, 4)
    ]

    def select_rows():
        table.wait()
        vocab_rows = table_hold.shape[0]
        tokens = token_ref.shape[0]
        columns = lax.broadcasted_iota(jnp.int32, (tokens, vocab_rows), 1)
        onehot = (token_ref[...] - r * vocab_rows == columns).astype(jnp.bfloat16)
        block = 256

        def select(i, carry):
            where = pl.ds(pl.multiple_of(i * block, block), block)
            rows_here = jnp.dot(
                onehot, table_hold[:, where], preferred_element_type=jnp.float32
            ).astype(jnp.bfloat16)
            part_ref[:, :, :, where] = rows_here.reshape(planes, 2, batch, block)
            return carry

        lax.fori_loop(0, feats // block, select, 0)

    def join():
        for copy in gives:
            copy.wait()
        for plane in range(planes):
            own = part_ref[plane, k].astype(jnp.float32)
            joined[plane] = (own + given[plane].astype(jnp.float32)).astype(jnp.bfloat16)

    def sum_picks():
        for copy in picks:
            copy.wait()
        total = joined[z].astype(jnp.float32)
        for far in range(1, planes):
            total = total + picked[far - 1].astype(jnp.float32)
        pieces[t] = total.astype(jnp.bfloat16)

    def normalise():
        for copy in gather:
            copy.wait()
        square = jnp.zeros((batch, 1), jnp.float32)
        for i in range(4):
            part = pieces[i].astype(jnp.float32)
            square = square + jnp.sum(part * part, axis=1, keepdims=True)
        factor = lax.rsqrt(square / (4 * feats) + 1e-05)
        for i in range(4):
            part = pieces[i].astype(jnp.float32)
            gain = gain_ref[:, i * feats : (i + 1) * feats].astype(jnp.float32)
            normed_ref[:, i * feats : (i + 1) * feats] = (part * factor * gain).astype(
                jnp.bfloat16
            )
        block = 256
        line = lax.broadcasted_iota(jnp.int32, (block, 2 * block), 0)
        column = lax.broadcasted_iota(jnp.int32, (block, 2 * block), 1)
        even = (column == 2 * line).astype(jnp.bfloat16)
        odd = (column == 2 * line + 1).astype(jnp.bfloat16)

        def spread(i, carry):
            part = normed_ref[:, pl.ds(pl.multiple_of(i * block, block), block)]
            where = pl.ds(pl.multiple_of(i * 2 * block, 2 * block), 2 * block)
            spread_ref[0:batch, where] = jnp.dot(
                part, even, preferred_element_type=jnp.float32
            ).astype(jnp.bfloat16)
            spread_ref[batch : 2 * batch, where] = jnp.dot(
                part, odd, preferred_element_type=jnp.float32
            ).astype(jnp.bfloat16)
            return carry

        lax.fori_loop(0, 4 * feats // block, spread, 0)

    steps = 4 * (planes - 1)
    for step in range(steps):
        if 0 < step < 4:
            pid = piece_id(z, k, other[step])
            landed(pid)
            onward(pid, stored(pid), step, True, True)
        far, j = step // 4 + 1, step % 4

        @pl.when(z >= far)
        def _():
            pid = piece_id(lax.rem(z + planes - far, planes), k, other[j])
            landed(pid)
            onward(pid, stored(pid), 4 * far + j, True, False)

        @pl.when(z + far < planes)
        def _():
            pid = piece_id(lax.rem(z + far, planes), k, other[j])
            landed(pid)
            onward(pid, stored(pid), 4 * (planes - 1 + far) + j, False, True)

        if step == 0:
            select_rows()
        if step == 1:
            for copy in gives:
                copy.start()
        if step == 2:
            join()
        if step == 3:
            for copy in picks:
                copy.start()
        if step == 7:
            sum_picks()
        if step == 8:
            for copy in gather:
                copy.start()
        if step == 9:
            normalise()

    for copy in put:
        copy.wait()
    for made in across:
        for copy in made:
            copy.wait_send()
    onward(mine, sources, 0, True, True, wait=True)
    for j in range(1, 4):
        pid = piece_id(z, k, other[j])
        onward(pid, stored(pid), j, True, True, wait=True)
    for step in range(steps):
        far, j = step // 4 + 1, step % 4

        @pl.when(z >= far)
        def _():
            pid = piece_id(lax.rem(z + planes - far, planes), k, other[j])
            onward(pid, stored(pid), 4 * far + j, True, False, wait=True)

        @pl.when(z + far < planes)
        def _():
            pid = piece_id(lax.rem(z + far, planes), k, other[j])
            onward(pid, stored(pid), 4 * (planes - 1 + far) + j, False, True, wait=True)

    for plane in range(planes):
        for j in range(4):
            landed(piece_id(plane, 1 - k, j))


def exchange(token_ids, norm_gain, embed_table, w_query, w_keyvalue, planes, batch):
    rows, all_query = w_query.shape
    query_cols, pair_cols = all_query // 4, w_keyvalue.shape[2] // 4
    replicas = 2 * planes
    width = rows * replicas * 4
    feats = embed_table.shape[1]
    kind = w_query.dtype
    anywhere = pl.BlockSpec(memory_space=pl.ANY)
    vmem = pl.BlockSpec(memory_space=pltpu.VMEM)
    hbm = pl.BlockSpec(memory_space=pltpu.HBM)
    dma = pltpu.SemaphoreType.DMA
    slots = 4 * (2 * planes - 1)
    return pl.pallas_call(
        functools.partial(exchange_kernel, planes),
        out_shape=(
            jax.ShapeDtypeStruct((width, query_cols), w_query.dtype),
            jax.ShapeDtypeStruct((width, 2, pair_cols), w_query.dtype),
            jax.ShapeDtypeStruct((batch, width), w_query.dtype),
            jax.ShapeDtypeStruct((2 * batch, 2 * width), w_query.dtype),
        ),
        in_specs=[vmem, vmem, hbm, hbm, hbm],
        out_specs=(anywhere, anywhere, vmem, vmem),
        scratch_shapes=[
            pltpu.VMEM((rows, query_cols), w_query.dtype),
            pltpu.VMEM((rows, 2, pair_cols), w_query.dtype),
            pltpu.VMEM(embed_table.shape, kind),
            pltpu.VMEM((planes, 2, batch, feats), kind),
            pltpu.VMEM((planes, batch, feats), kind),
            pltpu.VMEM((planes, batch, feats), kind),
            pltpu.VMEM((planes - 1, batch, feats), kind),
            pltpu.VMEM((4, batch, feats), kind),
            dma((2, 3, slots)),
            dma((2, replicas * 4)),
            dma((2, 3)),
            dma((5,)),
            dma((planes,)),
            dma((planes,)),
            dma((planes - 1,)),
            dma((planes - 1,)),
            dma((3,)),
            dma((3,)),
        ],
        compiler_params=pltpu.CompilerParams(
            collective_id=0, has_side_effects=True, vmem_limit_bytes=20 * 2**20
        ),
        cost_estimate=pl.CostEstimate(
            flops=2 * 10**11, bytes_accessed=2 * width * query_cols, transcendentals=0
        ),
        name="weight_exchange",
    )(token_ids.reshape(-1, 1), norm_gain.reshape(1, -1), embed_table, w_query, w_keyvalue)


def project_kernel(
    normed_ref,
    spread_ref,
    query_in,
    pair_in,
    query_all,
    pair_all,
    query_ref,
    pair_ref,
    q_ref,
    kv_ref,
    q_acc,
    kv_acc,
    sems,
):
    step = pl.program_id(0)
    stores = [
        pltpu.make_async_copy(query_all, query_ref, sems.at[0]),
        pltpu.make_async_copy(pair_all, pair_ref, sems.at[1]),
    ]

    @pl.when(step == 0)
    def _():
        for copy in stores:
            copy.start()
        q_acc[...] = jnp.zeros_like(q_acc)
        kv_acc[...] = jnp.zeros_like(kv_acc)

    q_acc[...] += jnp.dot(normed_ref[...], query_in[...], preferred_element_type=jnp.float32)
    kv_acc[...] += jnp.dot(spread_ref[...], pair_in[...], preferred_element_type=jnp.float32)

    @pl.when(step == pl.num_programs(0) - 1)
    def _():
        q_ref[...] = q_acc[...].astype(q_ref.dtype)
        kv_ref[...] = kv_acc[...].astype(kv_ref.dtype)
        for copy in stores:
            copy.wait()


def project(normed, spread, query_all, pair_all):
    batch, width = normed.shape
    query_cols, pair_cols = query_all.shape[1], pair_all.shape[2]
    pair_flat = pair_all.reshape(2 * width, pair_cols)
    block = 512
    anywhere = pl.BlockSpec(memory_space=pl.ANY)
    hbm = pl.BlockSpec(memory_space=pltpu.HBM)
    query_spec = pl.BlockSpec((block, query_cols), lambda i: (i, 0))
    pair_spec = pl.BlockSpec((2 * block, pair_cols), lambda i: (i, 0))
    query_out, pair_out, query, pair = pl.pallas_call(
        project_kernel,
        grid=(width // block,),
        out_shape=(
            jax.ShapeDtypeStruct(query_all.shape, query_all.dtype),
            jax.ShapeDtypeStruct(pair_flat.shape, pair_all.dtype),
            jax.ShapeDtypeStruct((batch, query_cols), normed.dtype),
            jax.ShapeDtypeStruct((2 * batch, pair_cols), normed.dtype),
        ),
        in_specs=[
            pl.BlockSpec((batch, block), lambda i: (0, i)),
            pl.BlockSpec((2 * batch, 2 * block), lambda i: (0, i)),
            query_spec,
            pair_spec,
            anywhere,
            anywhere,
        ],
        out_specs=(
            hbm,
            hbm,
            pl.BlockSpec((batch, query_cols), lambda i: (0, 0)),
            pl.BlockSpec((2 * batch, pair_cols), lambda i: (0, 0)),
        ),
        scratch_shapes=[
            pltpu.VMEM((batch, query_cols), jnp.float32),
            pltpu.VMEM((2 * batch, pair_cols), jnp.float32),
            pltpu.SemaphoreType.DMA((2,)),
        ],
        compiler_params=pltpu.CompilerParams(vmem_limit_bytes=16 * 2**20),
        cost_estimate=pl.CostEstimate(
            flops=2 * batch * width * (query_cols + 4 * pair_cols),
            bytes_accessed=4 * width * (query_cols + 2 * pair_cols),
            transcendentals=0,
        ),
        name="project_and_store",
    )(normed, spread, query_all, pair_flat, query_all, pair_flat)
    return query_out, pair_out.reshape(width, 2, pair_cols), query, pair


def per_device_line(
    planes,
    token_ids,
    embed_table,
    norm_gain,
    w_query,
    w_keyvalue,
    key_cache,
    value_cache,
    cache_lengths,
):
    batch = cache_lengths.shape[0]
    head_size = key_cache.shape[2]
    query_all, pair_all, normed, spread = exchange(
        token_ids, norm_gain, embed_table, w_query, w_keyvalue, planes, batch
    )
    query_out, pair_out, query, pair = project(normed, spread, query_all, pair_all)
    query = query.reshape(batch, -1, head_size)
    context = attend(query, key_cache, value_cache, pair[:batch], pair[batch:], cache_lengths)
    return context.reshape(batch, -1), query_out, pair_out


def solution(mesh):
    replicas, tp = mesh.shape["replica"], mesh.shape["tp"]

    def body(*args):
        key_cache, lengths, w_keyvalue = args[5], args[7], args[4]
        one_head = w_keyvalue.shape[2] == tp * key_cache.shape[2]
        own_rows = key_cache.shape[0] == lengths.shape[0]
        if tp == 4 and replicas % 2 == 0 and replicas > 6 and one_head and own_rows:
            return per_device_line(replicas // 2, *args)
        return per_device(*args)

    return jax.shard_map(
        body,
        mesh=mesh,
        in_specs=(
            P(),
            P("replica", "tp"),
            P(),
            P(("replica", "tp"), None),
            P(("replica", "tp"), None, None),
            P(("replica", "tp"), None, None),
            P(("replica", "tp"), None, None),
            P("replica"),
        ),
        out_specs=(P(("replica", "tp"), None), P(None, "tp"), P(None, None, "tp")),
        check_vma=False,
    )
```
